8 devices in a mesh: dp: 1 (over z), eo: 2 (over y), em: 2 (over x), ei: 2 (over core).
Axes of the slice: x: 2, y: 2, z: 1, core: 2. Of those that a mesh axis runs over, the one named last changes fastest.
Arguments:
- x_disp: bfloat16 [8, 64, 192, 2048], P('dp', ('eo', 'em', 'ei'))
- w_gate: bfloat16 [64, 2048, 1408], P(('eo', 'em', 'ei'))
- w_up: bfloat16 [64, 2048, 1408], P(('eo', 'em', 'ei'))
- w_down: bfloat16 [64, 1408, 2048], P(('eo', 'em', 'ei'))
- slot_idx: int32 [8192, 6], P(('dp', 'eo', 'em', 'ei'))
- expert_idx: int32 [8192, 6], P(('dp', 'eo', 'em', 'ei'))
- gate_wt: float32 [8192, 6], P(('dp', 'eo', 'em', 'ei'))
Outputs:
- output: bfloat16 [8192, 2048], P(('dp', 'eo', 'em', 'ei'))
All inputs are finite; a program needn't handle non-finite values.
Results may differ from the reference program's by a relative error of at most 0.00136.
Values are sent between devices in bfloat16 or wider.
A program may use at most 1 GiB of HBM per device.

```python
import jax
import jax.numpy as jnp
from jax import lax

D = 2048
FF = 1408
EXPERTS = 64
TOP = 6
TOK_DEV = 1024
GROUP = 8
SLOTS = 192
TOKENS = GROUP * TOK_DEV


def assign_slots(flat_ids):
    sort_order = jnp.argsort(flat_ids, stable=True)
    sorted_ids = flat_ids[sort_order]
    counts = jnp.bincount(flat_ids, length=EXPERTS)
    starts = jnp.cumsum(counts) - counts
    rank_sorted = jnp.arange(TOK_DEV * TOP) - starts[sorted_ids]
    slot_rank = jnp.zeros_like(rank_sorted).at[sort_order].set(rank_sorted)
    return jnp.where(slot_rank < SLOTS, slot_rank, -1).astype(jnp.int32)


def draw_routing(route_key):
    noise_key, bias_key, hot_key, shift_key = jax.random.split(route_key, 4)
    expert_ids = jnp.arange(EXPERTS, dtype=jnp.int32)
    popularity = jax.random.randint(bias_key, (EXPERTS,), 0, 48, dtype=jnp.int32)
    hot_expert = jax.random.randint(hot_key, (), 0, EXPERTS, dtype=jnp.int32)
    popularity = jnp.where(expert_ids == hot_expert, 100000, popularity)
    score_noise = jax.random.randint(noise_key, (TOKENS, EXPERTS), 0, 64, dtype=jnp.int32)
    route_score = (score_noise + popularity[None, :]) * EXPERTS + expert_ids[None, :]
    chosen = lax.top_k(route_score, TOP)[1]
    col_shift = jax.random.randint(shift_key, (TOKENS, 1), 0, TOP, dtype=jnp.int32)
    column = (jnp.arange(TOP, dtype=jnp.int32)[None, :] + col_shift) % TOP
    chosen = jnp.take_along_axis(chosen, column, axis=1).astype(jnp.int32)
    slot_idx = jax.vmap(assign_slots)(chosen.reshape(GROUP, TOK_DEV * TOP))
    return slot_idx.reshape(TOKENS, TOP), chosen


def setup_inputs(seed: int = 0, part: int = 0) -> dict:
    part_key = jax.random.fold_in(jax.random.key(seed), part)
    x_key, route_key, gate_key = jax.random.split(part_key, 3)
    wg_key, wu_key, wd_key = jax.random.split(jax.random.key(seed + 1), 3)
    x_disp = jax.random.normal(x_key, (GROUP, EXPERTS, SLOTS, D), jnp.float32).astype(jnp.bfloat16)
    w_gate = (jax.random.normal(wg_key, (EXPERTS, D, FF), jnp.float32) * D ** -0.5).astype(jnp.bfloat16)
    w_up = (jax.random.normal(wu_key, (EXPERTS, D, FF), jnp.float32) * D ** -0.5).astype(jnp.bfloat16)
    w_down = (jax.random.normal(wd_key, (EXPERTS, FF, D), jnp.float32) * (1.5 * FF ** -0.5)).astype(jnp.bfloat16)
    slot_idx, expert_idx = draw_routing(route_key)
    gate_wt = jax.nn.softmax(1.2 * jax.random.normal(gate_key, (TOKENS, TOP), jnp.float32), axis=-1)
    return {'x_disp': x_disp, 'w_gate': w_gate, 'w_up': w_up, 'w_down': w_down,
            'slot_idx': slot_idx, 'expert_idx': expert_idx, 'gate_wt': gate_wt}


def reference(x_disp, w_gate, w_up, w_down, slot_idx, expert_idx, gate_wt):
    def expert_rows(operands):
        x_rows, wg_e, wu_e, wd_e = operands
        flat_rows = x_rows.reshape(GROUP * SLOTS, D)
        gate_pre = jnp.dot(flat_rows, wg_e, preferred_element_type=jnp.float32)
        up_pre = jnp.dot(flat_rows, wu_e, preferred_element_type=jnp.float32)
        hidden = (jax.nn.silu(gate_pre) * up_pre).astype(jnp.bfloat16)
        y_flat = jnp.dot(hidden, wd_e, preferred_element_type=jnp.float32).astype(jnp.bfloat16)
        return y_flat.reshape(GROUP, SLOTS, D)

    y_rows = lax.map(expert_rows, (jnp.swapaxes(x_disp, 0, 1), w_gate, w_up, w_down))
    source = (jnp.arange(TOKENS, dtype=jnp.int32) // TOK_DEV)[:, None]
    is_live = slot_idx >= 0
    row_index = jnp.where(is_live, (expert_idx * GROUP + source) * SLOTS + slot_idx, 0)
    weight = jnp.where(is_live, gate_wt, 0.0)
    picked = jnp.take(y_rows.reshape(EXPERTS * GROUP * SLOTS, D), row_index, axis=0)
    combined = jnp.sum(weight[:, :, None] * picked.astype(jnp.float32), axis=1)
    return combined.astype(jnp.bfloat16)
```

```python
import functools

import jax
import jax.numpy as jnp
from jax import lax
from jax.experimental import pallas as pl
from jax.experimental.pallas import tpu as pltpu
from jax.sharding import PartitionSpec as P

GROUP_AXES = ('eo', 'em', 'ei')
LANES = 128
COLS = 1024
JT = COLS // LANES
ANY = pl.ANY


def token_address(tok):
    return (tok // 8) * (8 * JT) + tok % 8


def slot_tables(slot_idx, expert_idx, gate_wt, n_exp, n_slot):
    n_tok, top = slot_idx.shape
    tok = lax.broadcasted_iota(jnp.int32, (n_tok, top), 0)
    spare = float(n_tok * JT)
    delta = token_address(tok).astype(jnp.float32) - spare
    exp_hot = (expert_idx[:, :, None] == lax.broadcasted_iota(jnp.int32, (1, 1, n_exp), 2)).astype(jnp.float32)
    slot_hot = (slot_idx[:, :, None] == lax.broadcasted_iota(jnp.int32, (1, 1, n_slot), 2)).astype(jnp.float32)
    both = jnp.concatenate([exp_hot * delta[:, :, None], exp_hot * gate_wt[:, :, None]], axis=2)
    table = jnp.einsum('tje,tjc->ec', both, slot_hot, precision=lax.Precision.HIGHEST,
                       preferred_element_type=jnp.float32)
    addr, wt = table[:n_exp] + spare, table[n_exp:]
    return jnp.stack([addr, wt])


def gate_up_kernel(q_ref, x_ref, wg_ref, wu_ref, *rest):
    h_ref = rest[-1]
    _, _, slots, width = x_ref.shape
    ff = wg_ref.shape[2]

    def step(j, carry):
        cols = pl.ds(pl.multiple_of(j * LANES, LANES), LANES)
        w = jnp.concatenate([wg_ref[0, :, cols], wu_ref[0, :, cols]], axis=1)
        x = x_ref[...].reshape(2 * slots, width)
        gu = jnp.dot(x, w, preferred_element_type=jnp.float32)
        g, u = gu[:, :LANES], gu[:, LANES:]
        h = (g * jax.nn.sigmoid(g)) * u
        h_ref[0, :, :, cols] = h.astype(h_ref.dtype).reshape(2, slots, LANES)
        return carry

    lax.fori_loop(0, ff // LANES, step, 0)


def gate_up(q, x, wg, wu, after):
    n_src, n_exp, slots, width = x.shape
    ff = wg.shape[2]
    return pl.pallas_call(
        gate_up_kernel,
        grid_spec=pltpu.PrefetchScalarGridSpec(
            num_scalar_prefetch=1, grid=(n_exp,),
            in_specs=[pl.BlockSpec((2, 1, slots, width), lambda e, q: (q[0], e, 0, 0)),
                      pl.BlockSpec((1, width, ff), lambda e, q: (e, 0, 0)),
                      pl.BlockSpec((1, width, ff), lambda e, q: (e, 0, 0))] +
                     [pl.BlockSpec(memory_space=ANY)] * len(after),
            out_specs=pl.BlockSpec((1, 2, slots, ff), lambda e, q: (e, 0, 0, 0))),
        out_shape=jax.ShapeDtypeStruct((n_exp, 2, slots, ff), jnp.bfloat16),
        compiler_params=pltpu.CompilerParams(dimension_semantics=('arbitrary',), vmem_limit_bytes=60 * 2 ** 20),
        cost_estimate=pl.CostEstimate(flops=2 * n_exp * 2 * slots * width * ff * 2, transcendentals=0,
                                      bytes_accessed=n_exp * width * ff * 4),
        name='gate_up',
    )(q, x, wg, wu, *after)


def down_combine_kernel(sc_ref, addr_ref, wt_ref, n_ref, h0_ref, h1_ref, wd_ref, *rest):
    own_ref, sib_ref, y_ref = rest[-3:]
    e = pl.program_id(0)
    n_exp = pl.num_programs(0)
    slots = h0_ref.shape[2]

    @pl.when(e == 0)
    def _():
        rows = own_ref.shape[0]

        def zero(i, carry):
            z = jnp.zeros((8 * JT, LANES), jnp.float32)
            r = pl.ds(pl.multiple_of(i * 8 * JT, 8 * JT), 8 * JT)
            own_ref[r, :] = z
            sib_ref[r, :] = z
            return carry

        lax.fori_loop(0, rows // (8 * JT), zero, 0)

    for i, h_ref in enumerate((h0_ref, h1_ref)):
        for jj in range(COLS // 256):
            y = jnp.dot(h_ref[0, 0], wd_ref[0, :, jj * 256:(jj + 1) * 256], preferred_element_type=jnp.float32)
            y = y.astype(jnp.bfloat16).astype(jnp.float32)
            for k in range(2):
                y_ref[i, :, (jj * 2 + k) * 8:(jj * 2 + k + 1) * 8, :] = (
                    y[:, k * LANES:(k + 1) * LANES].reshape(slots // 8, 8, LANES))

    for i, acc_ref in enumerate((own_ref, sib_ref)):
        se = (2 * sc_ref[0] + (sc_ref[1] if i == 0 else 1 - sc_ref[1])) * n_exp + e
        base = se * slots
        yi = y_ref.at[i]

        def batch(b, carry):
            addrs = [addr_ref[base + b * 8 + k] for k in range(8)]
            wts = [wt_ref[base + b * 8 + k] for k in range(8)]
            ys = [yi[b, pl.ds(k, JT, stride=8), :] for k in range(8)]
            old = [acc_ref[pl.ds(addrs[k], JT, stride=8), :] for k in range(8)]
            new = [old[k] + wts[k] * ys[k] for k in range(8)]
            for k in range(8):
                acc_ref[pl.ds(addrs[k], JT, stride=8), :] = new[k]
            return carry

        lax.fori_loop(0, (n_ref[se] + 7) // 8, batch, 0)


def down_combine(sc, addr, wt, count, h, wd, n, n_tok, after):
    n_exp, _, slots, ff = h.shape
    rows = (n_tok + 8) * JT
    acc = jax.ShapeDtypeStruct((rows, LANES), jnp.float32)
    return pl.pallas_call(
        down_combine_kernel,
        grid_spec=pltpu.PrefetchScalarGridSpec(
            num_scalar_prefetch=4, grid=(n_exp,),
            in_specs=[pl.BlockSpec((1, 1, slots, ff), lambda e, sc, a, w, c: (e, sc[1], 0, 0)),
                      pl.BlockSpec((1, 1, slots, ff), lambda e, sc, a, w, c: (e, 1 - sc[1], 0, 0)),
                      pl.BlockSpec((1, ff, COLS), lambda e, sc, a, w, c: (e, 0, n))] +
                     [pl.BlockSpec(memory_space=ANY)] * len(after),
            out_specs=[pl.BlockSpec((rows, LANES), lambda e, sc, a, w, c: (0, 0))] * 2,
            scratch_shapes=[pltpu.VMEM((2, slots // 8, 8 * JT, LANES), jnp.float32)]),
        out_shape=[acc, acc],
        compiler_params=pltpu.CompilerParams(dimension_semantics=('arbitrary',), vmem_limit_bytes=60 * 2 ** 20),
        cost_estimate=pl.CostEstimate(flops=2 * n_exp * 2 * slots * ff * COLS * 2, transcendentals=0,
                                      bytes_accessed=n_exp * COLS * ff * 2 + 2 * rows * LANES * 4),
        name='down_combine',
    )(sc, addr, wt, count, h, h, wd, *after)


def final_kernel(*refs):
    out_ref = refs[-1]
    ins = refs[:-1]
    n_cb = len(ins) // 6
    step = pl.program_id(0)
    half = pl.num_programs(0) // 2
    blocks = out_ref.shape[0] // 16

    def emit(lower):
        def body(b, carry):
            r = pl.ds(pl.multiple_of(b * 16 * JT, 16 * JT), 16 * JT)
            for n in range(n_cb):
                own, sib, x1, x2, y1, y2 = ins[6 * n:6 * n + 6]
                xr, yr = (x1, y1) if lower else (x2, y2)
                s = (own[r, :] + sib[r, :]) + (xr[r, :] + yr[r, :])
                s = s.reshape(2, JT, 8, LANES)
                for j in range(JT):
                    col = n * COLS + j * LANES
                    out_ref[pl.ds(pl.multiple_of(b * 16, 16), 16), col:col + LANES] = (
                        s[:, j].reshape(16, LANES).astype(out_ref.dtype))
            return carry

        lax.fori_loop(0, blocks, body, 0)

    pl.when(step < half)(lambda: emit(True))
    pl.when(step >= half)(lambda: emit(False))


def final_sum(parts, n_tok, width):
    tb = 64
    steps = n_tok // tb
    half = steps // 2
    blk = tb * JT
    full = pl.BlockSpec((blk, LANES), lambda i: (i, 0))
    low = pl.BlockSpec((blk, LANES), lambda i: (jnp.minimum(i, half - 1), 0))
    high = pl.BlockSpec((blk, LANES), lambda i: (jnp.maximum(i - half, 0), 0))
    flat = [a for p in parts for a in p]
    return pl.pallas_call(
        final_kernel,
        grid=(steps,),
        in_specs=[full, full, low, high, low, high] * len(parts),
        out_specs=pl.BlockSpec((tb, width), lambda i: (i, 0)),
        out_shape=jax.ShapeDtypeStruct((n_tok, width), jnp.bfloat16),
        compiler_params=pltpu.CompilerParams(dimension_semantics=('arbitrary',), vmem_limit_bytes=40 * 2 ** 20),
        cost_estimate=pl.CostEstimate(flops=10 ** 7, transcendentals=0, bytes_accessed=n_tok * width * 18),
        name='final_sum',
    )(*flat)


def solution(mesh):
    token_spec = P(('dp',) + GROUP_AXES, None)
    weight_spec = P(GROUP_AXES, None, None)
    rows_spec = P('dp', GROUP_AXES, None, None)
    n_dev = mesh.shape['eo'] * mesh.shape['em'] * mesh.shape['ei']

    def swap(a, bit):
        return lax.ppermute(a, GROUP_AXES, [(i, i ^ bit) for i in range(n_dev)])

    def local_part(x_local, w_gate, w_up, w_down, slot_idx, expert_idx, gate_wt):
        n_src, n_exp, slots, width = x_local.shape
        n_tok = slot_idx.shape[0]
        n_cb = width // COLS
        core = lax.axis_index('ei')
        chip = lax.axis_index('eo') * 2 + lax.axis_index('em')

        table = slot_tables(slot_idx, expert_idx, gate_wt, n_dev * n_exp, slots)
        table = table.reshape(2, n_dev, n_exp, slots).swapaxes(0, 1)
        table = lax.all_to_all(table, GROUP_AXES, 0, 0, tiled=True)
        addr = table[:, 0].astype(jnp.int32)
        wt = table[:, 1]
        seen = jnp.where(wt > 0, lax.broadcasted_iota(jnp.int32, wt.shape, 2) + 1, 0)
        count = jnp.max(seen, axis=2).reshape(-1)
        addr, wt = addr.reshape(-1), wt.reshape(-1)

        def ffn(flip, after):
            q = chip ^ flip
            h = gate_up(q.astype(jnp.int32).reshape(1), x_local, w_gate, w_up, after)
            sc = jnp.stack([q, core]).astype(jnp.int32)
            own, sib = [], []
            prev = []
            for n in range(n_cb):
                o, s = down_combine(sc, addr, wt, count, h, w_down, n, n_tok, prev)
                own.append(o)
                sib.append(swap(s, 1))
                prev = [o]
            return own, sib

        lo, hi = slice(0, n_tok // 2 * JT), slice(n_tok // 2 * JT, n_tok * JT)
        own, sib = ffn(3, [])
        relay_x, relay_y, gate = [], [], []
        for n in range(n_cb):
            s1 = own[n][lo] + sib[n][lo]
            s2 = own[n][hi] + sib[n][hi]
            relay_x.append(swap(s1, 2))
            relay_y.append(swap(s2, 4))
            gate += [s1]
        own_x, sib_x = ffn(1, gate)
        got_x1 = [swap(own_x[n][lo] + sib_x[n][lo], 2) for n in range(n_cb)]
        own_y, sib_y = ffn(2, [own_x[-1]])
        got_y2 = [swap(own_y[n][hi] + sib_y[n][hi], 4) for n in range(n_cb)]
        got_x2 = [swap(own_x[n][hi] + sib_x[n][hi] + relay_y[n], 2) for n in range(n_cb)]
        got_y1 = [swap(own_y[n][lo] + sib_y[n][lo] + relay_x[n], 4) for n in range(n_cb)]
        own_o, sib_o = ffn(0, [own_y[-1]])
        parts = [(own_o[n], sib_o[n], got_x1[n], got_x2[n], got_y1[n], got_y2[n]) for n in range(n_cb)]
        return final_sum(parts, n_tok, width)

    return jax.shard_map(local_part, mesh=mesh,
                         in_specs=(rows_spec, weight_spec, weight_spec, weight_spec, token_spec, token_spec, token_spec),
                         out_specs=token_spec, check_vma=False)
```

```python
import functools

import jax
import jax.numpy as jnp
from jax import lax
from jax.experimental import pallas as pl
from jax.experimental.pallas import tpu as pltpu
from jax.sharding import PartitionSpec as P


GROUP_AXES = ('eo', 'em', 'ei')
LANES = 128
COLS = 1024
JT = COLS // LANES
ANY = pl.ANY


def slot_tables(slot_idx, expert_idx, gate_wt, n_exp, n_slot):
    n_tok, top = slot_idx.shape
    tok = lax.broadcasted_iota(jnp.int32, (n_tok, top), 0)
    spare = float(n_tok * JT)
    delta = (tok * JT).astype(jnp.float32) - spare
    exp_hot = (expert_idx[:, :, None] == lax.broadcasted_iota(jnp.int32, (1, 1, n_exp), 2)).astype(jnp.float32)
    slot_hot = (slot_idx[:, :, None] == lax.broadcasted_iota(jnp.int32, (1, 1, n_slot), 2)).astype(jnp.float32)
    both = jnp.concatenate([exp_hot * delta[:, :, None], exp_hot * gate_wt[:, :, None]], axis=2)
    table = jnp.einsum('tje,tjc->ec', both, slot_hot, precision=lax.Precision.HIGHEST,
                       preferred_element_type=jnp.float32)
    addr, wt = table[:n_exp] + spare, table[n_exp:]
    return jnp.stack([addr, wt])


def round16(n):
    return (n + 15) // 16 * 16


def row_chunks(total, body):
    whole = (total + 127) // 256
    rest = total - whole * 256

    def chunk(c, carry):
        body(pl.multiple_of(c * 256, 256), 256)
        return carry

    lax.fori_loop(0, whole, chunk, 0)
    pl.when(rest > 0)(lambda: body(pl.multiple_of(whole * 256, 256), 128))


def gate_up_tile(x, wg_ref, wu_ref, cols):
    w = jnp.concatenate([wg_ref[0, :, cols], wu_ref[0, :, cols]], axis=1)
    gu = jnp.dot(x, w, preferred_element_type=jnp.float32)
    g, u = gu[:, :LANES], gu[:, LANES:]
    return ((g * jax.nn.sigmoid(g)) * u).astype(jnp.bfloat16)


def gate_up_full_kernel(q_ref, x_ref, wg_ref, wu_ref, h_ref):
    _, _, slots, width = x_ref.shape
    for j in range(wg_ref.shape[2] // LANES):
        cols = slice(j * LANES, (j + 1) * LANES)
        h_ref[0, :, cols] = gate_up_tile(x_ref[...].reshape(2 * slots, width), wg_ref, wu_ref, cols)


def gate_up_full(q, x, wg, wu):
    _, n_exp, slots, width = x.shape
    ff = wg.shape[2]
    return pl.pallas_call(
        gate_up_full_kernel,
        grid_spec=pltpu.PrefetchScalarGridSpec(
            num_scalar_prefetch=1, grid=(n_exp,),
            in_specs=[pl.BlockSpec((2, 1, slots, width), lambda e, q: (q[0], e, 0, 0))] +
                     [pl.BlockSpec((1, width, ff), lambda e, q: (e, 0, 0))] * 2,
            out_specs=pl.BlockSpec((1, 2 * slots, ff), lambda e, q: (e, 0, 0))),
        out_shape=jax.ShapeDtypeStruct((n_exp, 2 * slots, ff), jnp.bfloat16),
        compiler_params=pltpu.CompilerParams(dimension_semantics=('arbitrary',), vmem_limit_bytes=60 * 2 ** 20),
        cost_estimate=pl.CostEstimate(flops=2 * n_exp * 2 * slots * width * ff * 2, transcendentals=0,
                                      bytes_accessed=n_exp * width * ff * 4),
        name='gate_up_full',
    )(q, x, wg, wu)


def gate_up_kernel(n_q, q_ref, n_ref, *refs):
    x_refs, (wg_ref, wu_ref), (h_ref, xs_ref) = refs[:n_q], refs[n_q:n_q + 2], refs[-2:]
    e = pl.program_id(0)
    n_exp = pl.num_programs(0)
    ff = wg_ref.shape[2]

    first = jnp.int32(0)
    for g in range(n_q):
        for i in range(2):
            rows = round16(n_ref[(2 * q_ref[g] + i) * n_exp + e])
            at = first

            def copy(b, carry):
                xs_ref[pl.ds(pl.multiple_of(at + b * 16, 16), 16), :] = (
                    x_refs[g][i, 0, pl.ds(pl.multiple_of(b * 16, 16), 16), :])
                return carry

            lax.fori_loop(0, rows // 16, copy, 0)
            first = first + rows

    def body(r0, rows):
        r = pl.ds(r0, rows)
        for j in range(ff // LANES):
            cols = slice(j * LANES, (j + 1) * LANES)
            h_ref[0, r, cols] = gate_up_tile(xs_ref[r, :], wg_ref, wu_ref, cols)

    row_chunks(first, body)


def gate_up(qs, count, x, wg, wu, after):
    _, n_exp, slots, width = x.shape
    ff = wg.shape[2]
    n_q = qs.shape[0]
    rows = n_q * 2 * slots

    def x_spec(g):
        return pl.BlockSpec((2, 1, slots, width), lambda e, q, c: (q[g], e, 0, 0))

    return pl.pallas_call(
        functools.partial(gate_up_kernel, n_q),
        grid_spec=pltpu.PrefetchScalarGridSpec(
            num_scalar_prefetch=2, grid=(n_exp,),
            in_specs=[x_spec(g) for g in range(n_q)] +
                     [pl.BlockSpec((1, width, ff), lambda e, q, c: (e, 0, 0))] * 2 +
                     [pl.BlockSpec(memory_space=ANY)] * len(after),
            out_specs=pl.BlockSpec((1, rows, ff), lambda e, q, c: (e, 0, 0)),
            scratch_shapes=[pltpu.VMEM((rows, width), jnp.bfloat16)]),
        out_shape=jax.ShapeDtypeStruct((n_exp, rows, ff), jnp.bfloat16),
        compiler_params=pltpu.CompilerParams(dimension_semantics=('arbitrary',), vmem_limit_bytes=60 * 2 ** 20),
        cost_estimate=pl.CostEstimate(flops=2 * n_exp * rows * width * ff * 2, transcendentals=0,
                                      bytes_accessed=n_exp * width * ff * 4),
        name='gate_up',
    )(qs, count, *[x] * n_q, wg, wu, *after)


def down_combine_kernel(n_q, packed, q_ref, core_ref, n_ref, *refs):
    addr_refs, wt_refs, (h_ref, wd_ref), rest = refs[:n_q], refs[n_q:2 * n_q], refs[2 * n_q:2 * n_q + 2], refs[2 * n_q + 2:]
    outs, (acc_ref, y_ref, sem) = rest[-3 - 2 * n_q:-3], rest[-3:]
    e = pl.program_id(0)
    n_exp = pl.num_programs(0)
    n_acc = 2 * n_q
    slots = h_ref.shape[1] // n_acc

    @pl.when(e == 0)
    def _():
        def zero(i, carry):
            z = jnp.zeros((8 * JT, LANES), jnp.float32)
            r = pl.ds(pl.multiple_of(i * 8 * JT, 8 * JT), 8 * JT)
            for k in range(n_acc):
                acc_ref[k, r, :] = z
            return carry

        lax.fori_loop(0, acc_ref.shape[1] // (8 * JT), zero, 0)

    starts, counts = [], []
    first = jnp.int32(0)
    for g in range(n_q):
        for i in range(2):
            n = n_ref[(2 * q_ref[g] + i) * n_exp + e]
            starts.append(first)
            counts.append(n)
            first = first + (round16(n) if packed else slots)

    def body(r0, rows):
        for jj in range(COLS // 256):
            y = jnp.dot(h_ref[0, pl.ds(r0, rows), :], wd_ref[0, :, jj * 256:(jj + 1) * 256],
                        preferred_element_type=jnp.float32)
            y = y.astype(jnp.bfloat16).astype(jnp.float32)
            for k in range(2):
                y_ref[pl.ds(r0 // 8, rows // 8), (jj * 2 + k) * 8:(jj * 2 + k + 1) * 8, :] = (
                    y[:, k * LANES:(k + 1) * LANES].reshape(rows // 8, 8, LANES))

    if packed:
        row_chunks(first, body)
    else:
        body(0, n_acc * slots)

    for g in range(n_q):
        for i in range(2):
            k_acc = 2 * g + i
            y0 = starts[k_acc] // 8
            acc = acc_ref.at[k_acc]

            def batch(b, carry):
                ks = range(16)
                addrs = [addr_refs[g][0, 0, 0, i * slots + b * 16 + k] for k in ks]
                wts = [wt_refs[g][0, 0, 0, i * slots + b * 16 + k] for k in ks]
                ys = [y_ref[y0 + b * 2 + k // 8, pl.ds(k % 8, JT, stride=8), :] for k in ks]
                at = [pl.ds(pl.multiple_of(addrs[k], JT), JT) for k in ks]
                old = [acc[at[k], :] for k in ks]
                for k in ks:
                    acc[at[k], :] = old[k] + wts[k] * ys[k]
                return carry

            lax.fori_loop(0, (counts[k_acc] + 15) // 16, batch, 0)

    @pl.when(e == n_exp - 1)
    def _():
        copies = []
        for g in range(n_q):
            for i in range(2):
                own = core_ref[0] == i
                for dst, cond in ((outs[2 * g], own), (outs[2 * g + 1], jnp.logical_not(own))):
                    copy = pltpu.make_async_copy(acc_ref.at[2 * g + i], dst, sem.at[2 * g + i])
                    pl.when(cond)(copy.start)
                copies.append(copy)
        for copy in copies:
            copy.wait()


def down_combine(qs, core, addr, wt, count, h, wd, n, n_tok, slots, packed, after):
    n_exp, rows, ff = h.shape
    n_q = qs.shape[0]
    acc_rows = (n_tok + 8) * JT
    acc = jax.ShapeDtypeStruct((acc_rows, LANES), jnp.float32)

    def table_spec(g):
        return pl.BlockSpec((1, 1, 1, 2 * slots), lambda e, q, *_: (q[g], e, 0, 0), memory_space=pltpu.SMEM)

    return pl.pallas_call(
        functools.partial(down_combine_kernel, n_q, packed),
        grid_spec=pltpu.PrefetchScalarGridSpec(
            num_scalar_prefetch=3, grid=(n_exp,),
            in_specs=[table_spec(g) for g in range(n_q)] * 2 +
                     [pl.BlockSpec((1, rows, ff), lambda e, *_: (e, 0, 0)),
                      pl.BlockSpec((1, ff, COLS), lambda e, *_: (e, 0, n))] +
                     [pl.BlockSpec(memory_space=ANY)] * len(after),
            out_specs=[pl.BlockSpec(memory_space=ANY)] * (2 * n_q),
            scratch_shapes=[pltpu.VMEM((2 * n_q, acc_rows, LANES), jnp.float32),
                            pltpu.VMEM((rows // 8, 8 * JT, LANES), jnp.float32),
                            pltpu.SemaphoreType.DMA((2 * n_q,))]),
        out_shape=[acc] * (2 * n_q),
        compiler_params=pltpu.CompilerParams(dimension_semantics=('arbitrary',), vmem_limit_bytes=60 * 2 ** 20),
        cost_estimate=pl.CostEstimate(flops=2 * n_exp * rows * ff * COLS, transcendentals=0,
                                      bytes_accessed=n_exp * COLS * ff * 2 + 2 * n_q * acc_rows * LANES * 4),
        name='down_combine',
    )(qs, core, count, *[addr] * n_q, *[wt] * n_q, h, wd, *after)


def final_kernel(a1_ref, a2_ref, b1_ref, b2_ref, *rest):
    out_ref, s_ref = rest[-2:]
    step = pl.program_id(0)
    half = pl.num_programs(0) // 2

    def emit(a_ref, b_ref):
        def body(b, carry):
            r = pl.ds(pl.multiple_of(b * 16 * JT, 16 * JT), 16 * JT)
            s_ref[r, :] = a_ref[r, :] + b_ref[r, :]
            for j in range(JT):
                pair = [s_ref[pl.ds((b * 16 + k) * JT + j, 8, stride=JT), :] for k in (0, 8)]
                out_ref[pl.ds(pl.multiple_of(b * 16, 16), 16), j * LANES:(j + 1) * LANES] = (
                    jnp.concatenate(pair, axis=0).astype(out_ref.dtype))
            return carry

        lax.fori_loop(0, out_ref.shape[0] // 16, body, 0)

    pl.when(step < half)(lambda: emit(a1_ref, b1_ref))
    pl.when(step >= half)(lambda: emit(a2_ref, b2_ref))


def final_sum(a1, a2, b1, b2, n, n_tok, width, out):
    tb = 128
    steps = n_tok // tb
    half = steps // 2
    low = pl.BlockSpec((tb * JT, LANES), lambda i: (jnp.minimum(i, half - 1), 0))
    high = pl.BlockSpec((tb * JT, LANES), lambda i: (jnp.maximum(i - half, 0), 0))
    prior = [] if out is None else [out]
    return pl.pallas_call(
        final_kernel,
        grid=(steps,),
        in_specs=[low, high, low, high] + [pl.BlockSpec(memory_space=ANY)] * len(prior),
        out_specs=pl.BlockSpec((tb, COLS), lambda i: (i, n)),
        scratch_shapes=[pltpu.VMEM((tb * JT, LANES), jnp.float32)],
        out_shape=jax.ShapeDtypeStruct((n_tok, width), jnp.bfloat16),
        input_output_aliases={4: 0} if prior else {},
        compiler_params=pltpu.CompilerParams(dimension_semantics=('arbitrary',), vmem_limit_bytes=30 * 2 ** 20),
        cost_estimate=pl.CostEstimate(flops=10 ** 7, transcendentals=0, bytes_accessed=n_tok * COLS * 10),
        name='final_sum',
    )(a1, a2, b1, b2, *prior)


def solution(mesh):
    token_spec = P(('dp',) + GROUP_AXES, None)
    weight_spec = P(GROUP_AXES, None, None)
    rows_spec = P('dp', GROUP_AXES, None, None)
    n_dev = mesh.shape['eo'] * mesh.shape['em'] * mesh.shape['ei']
    core_bit, x_bit, y_bit = 1, 2, 4

    def swap(a, bit):
        return lax.ppermute(a, GROUP_AXES, [(i, i ^ bit) for i in range(n_dev)])

    def local_part(x_local, w_gate, w_up, w_down, slot_idx, expert_idx, gate_wt):
        _, n_exp, slots, width = x_local.shape
        n_tok = slot_idx.shape[0]
        n_cb = width // COLS
        core = lax.axis_index('ei').astype(jnp.int32).reshape(1)
        chip = (lax.axis_index('eo') * 2 + lax.axis_index('em')).astype(jnp.int32)

        table = slot_tables(slot_idx, expert_idx, gate_wt, n_dev * n_exp, slots)
        table = table.reshape(2, n_dev, n_exp, slots).swapaxes(0, 1)
        table = lax.all_to_all(table, GROUP_AXES, 0, 0, tiled=True)
        addr = table[:, 0].astype(jnp.int32)
        wt = table[:, 1]
        seen = jnp.where(wt > 0, lax.broadcasted_iota(jnp.int32, wt.shape, 2) + 1, 0)
        count = jnp.max(seen, axis=2).reshape(-1)

        def by_chip(a):
            return a.reshape(n_dev // 2, 2, n_exp, slots).swapaxes(1, 2).reshape(n_dev // 2, n_exp, 1, 2 * slots)

        addr, wt = by_chip(addr), by_chip(wt)

        lo, hi = slice(0, n_tok // 2 * JT), slice(n_tok // 2 * JT, n_tok * JT)
        blocks = range(n_cb)

        def ffn(flips, packed, after):
            qs = jnp.stack([chip ^ f for f in flips])
            if packed:
                h = gate_up(qs, count, x_local, w_gate, w_up, after)
            else:
                h = gate_up_full(qs, x_local, w_gate, w_up)
            outs = []
            prev = []
            for n in blocks:
                accs = down_combine(qs, core, addr, wt, count, h, w_down, n, n_tok, slots, packed, prev)
                outs.append([(accs[2 * g], swap(accs[2 * g + 1], core_bit))
                             for g in range(len(flips))])
                prev = [accs[0]]
            return outs

        diag = ffn([3], False, [])
        relay_x, relay_y, gate = [], [], []
        for n in blocks:
            (own, sib), = diag[n]
            first, second = own[lo] + sib[lo], own[hi] + sib[hi]
            relay_x.append(swap(first, x_bit))
            relay_y.append(swap(second, y_bit))
            gate.append(first)

        near = ffn([1, 2], True, gate)
        x1, x2, y1, y2 = [], [], [], []
        for n in blocks:
            (own_x, sib_x), (own_y, sib_y) = near[n]
            x1.append(swap(own_x[lo] + sib_x[lo], x_bit))
            y2.append(swap(own_y[hi] + sib_y[hi], y_bit))
            own_x, sib_x, own_y, sib_y, from_x, from_y = lax.optimization_barrier(
                (own_x, sib_x, own_y, sib_y, relay_x[n], relay_y[n]))
            x2.append(swap(own_x[hi] + sib_x[hi] + from_y, x_bit))
            y1.append(swap(own_y[lo] + sib_y[lo] + from_x, y_bit))

        here = ffn([0], True, [near[-1][0][0]])
        out = None
        for n in blocks:
            (own, sib), = here[n]
            a1 = own[lo] + sib[lo] + x1[n]
            a2 = own[hi] + sib[hi] + y2[n]
            out = final_sum(a1, a2, y1[n], x2[n], n, n_tok, width, out)
        return out

    return jax.shard_map(local_part, mesh=mesh,
                         in_specs=(rows_spec, weight_spec, weight_spec, weight_spec, token_spec, token_spec, token_spec),
                         out_specs=token_spec, check_vma=False)
```

```python
import jax
import jax.numpy as jnp
from jax import lax
from jax.experimental import pallas as pl
from jax.experimental.pallas import tpu as pltpu
from jax.sharding import PartitionSpec as P


GROUP_AXES = ('eo', 'em', 'ei')
LANES = 128
COLS = 1024
JT = COLS // LANES
ANY = pl.ANY


def slot_tables(slot_idx, expert_idx, gate_wt, n_exp, n_slot):
    n_tok, top = slot_idx.shape
    tok = lax.broadcasted_iota(jnp.int32, (n_tok, top), 0)
    spare = float(n_tok * JT)
    delta = (tok * JT).astype(jnp.float32) - spare
    exp_hot = (expert_idx[:, :, None] == lax.broadcasted_iota(jnp.int32, (1, 1, n_exp), 2)).astype(jnp.float32)
    slot_hot = (slot_idx[:, :, None] == lax.broadcasted_iota(jnp.int32, (1, 1, n_slot), 2)).astype(jnp.float32)
    both = jnp.concatenate([exp_hot * delta[:, :, None], exp_hot * gate_wt[:, :, None]], axis=2)
    table = jnp.einsum('tje,tjc->ec', both, slot_hot, precision=lax.Precision.HIGHEST,
                       preferred_element_type=jnp.float32)
    addr, wt = table[:n_exp] + spare, table[n_exp:]
    return jnp.stack([addr, wt])


def round16(n):
    return (n + 15) // 16 * 16


def row_chunks(total, body):
    whole = (total + 127) // 256
    rest = total - whole * 256

    def chunk(c, carry):
        body(pl.multiple_of(c * 256, 256), 256)
        return carry

    lax.fori_loop(0, whole, chunk, 0)
    pl.when(rest > 0)(lambda: body(pl.multiple_of(whole * 256, 256), 128))


def gate_up_tile(x, wg_ref, wu_ref, cols):
    w = jnp.concatenate([wg_ref[:, cols], wu_ref[:, cols]], axis=1)
    gu = jnp.dot(x, w, preferred_element_type=jnp.float32)
    g, u = gu[:, :LANES], gu[:, LANES:]
    return ((g * jax.nn.sigmoid(g)) * u).astype(jnp.bfloat16)


def pass_kernel(src_ref, core_ref, n_ref, *refs):
    x_refs, addr_refs, wt_refs, weights = refs[0:2], refs[2:4], refs[4:6], refs[6:9]
    outs, bufs, (h_ref, xs_ref, y_ref, acc_ref, w_sem, sem) = refs[-13:-9], refs[-9:-6], refs[-6:]
    ff = h_ref.shape[1]
    e = pl.program_id(0)
    n_exp = pl.num_programs(0)
    slot = e % 2

    def fetch(k, expert, into):
        return pltpu.make_async_copy(weights[k].at[expert], bufs[k].at[into], w_sem.at[into, k])

    @pl.when(e == 0)
    def _():
        for k in range(3):
            fetch(k, 0, 0).start()

    @pl.when(e + 1 < n_exp)
    def _():
        for k in range(3):
            fetch(k, e + 1, 1 - slot).start()

    @pl.when(e == 0)
    def _():
        def zero(i, carry):
            r = pl.ds(pl.multiple_of(i * 8 * JT, 8 * JT), 8 * JT)
            for k in range(acc_ref.shape[0]):
                acc_ref[k, r, :] = jnp.zeros((8 * JT, LANES), jnp.float32)
            return carry

        lax.fori_loop(0, acc_ref.shape[1] // (8 * JT), zero, 0)

    counts = [n_ref[src_ref[i] * n_exp + e] for i in range(2)]
    first = [jnp.int32(0), round16(counts[0])]
    total = first[1] + round16(counts[1])

    for i in range(2):
        def copy(b, carry):
            xs_ref[pl.ds(pl.multiple_of(first[i] + b * 16, 16), 16), :] = (
                x_refs[i][0, 0, pl.ds(pl.multiple_of(b * 16, 16), 16), :])
            return carry

        lax.fori_loop(0, round16(counts[i]) // 16, copy, 0)

    fetch(0, e, slot).wait()
    fetch(1, e, slot).wait()
    wg_ref, wu_ref, wd_ref = (buf.at[slot] for buf in bufs)

    def hidden(r0, rows):
        r = pl.ds(r0, rows)
        for j in range(ff // LANES):
            cols = slice(j * LANES, (j + 1) * LANES)
            h_ref[r, cols] = gate_up_tile(xs_ref[r, :], wg_ref, wu_ref, cols)

    row_chunks(total, hidden)
    fetch(2, e, slot).wait()

    def result(r0, rows):
        for jj in range(wd_ref.shape[1] // 256):
            y = jnp.dot(h_ref[pl.ds(r0, rows), :], wd_ref[:, jj * 256:(jj + 1) * 256],
                        preferred_element_type=jnp.float32)
            y = y.astype(jnp.bfloat16).astype(jnp.float32)
            for k in range(2):
                y_ref[pl.ds(r0 // 8, rows // 8), (jj * 2 + k) * 8:(jj * 2 + k + 1) * 8, :] = (
                    y[:, k * LANES:(k + 1) * LANES].reshape(rows // 8, 8, LANES))

    row_chunks(total, result)

    for i in range(2):
        y0 = first[i] // 8

        def batch(b, carry):
            at = [pl.ds(pl.multiple_of(addr_refs[i][0, 0, 0, b * 8 + k], JT), JT) for k in range(8)]
            wts = [wt_refs[i][0, 0, 0, b * 8 + k] for k in range(8)]
            work = [(k, col) for k in range(8) for col in range(2)]
            ys = [y_ref[y0 + b, pl.ds(col * 8 * JT + k, JT, stride=8), :] for k, col in work]
            old = [acc_ref[col * 2 + i, at[k], :] for k, col in work]
            for (k, col), y, a in zip(work, ys, old):
                acc_ref[col * 2 + i, at[k], :] = a + wts[k] * y
            return carry

        lax.fori_loop(0, (counts[i] + 7) // 8, batch, 0)

    @pl.when(e == n_exp - 1)
    def _():
        copies = []
        for col in range(2):
            for i in range(2):
                own = core_ref[0] == i
                k = col * 2 + i
                for dst, cond in ((outs[col * 2], own), (outs[col * 2 + 1], jnp.logical_not(own))):
                    copies.append((cond, pltpu.make_async_copy(acc_ref.at[k], dst, sem.at[k])))
        for cond, copy in copies:
            pl.when(cond)(copy.start)
        for cond, copy in copies:
            pl.when(cond)(copy.wait)


def ffn_pass(src, core, count, addr, wt, x, wg, wu, wd, n_tok, after):
    _, n_exp, slots, width = x.shape
    ff = wg.shape[2]
    rows = 2 * slots
    acc_rows = (n_tok + 8) * JT
    acc = jax.ShapeDtypeStruct((acc_rows, LANES), jnp.float32)
    x_specs = [pl.BlockSpec((1, 1, slots, width), lambda e, src, *_, i=i: (src[i], e, 0, 0)) for i in range(2)]
    table_specs = [pl.BlockSpec((1, 1, 1, slots), lambda e, src, *_, i=i: (src[i], e, 0, 0),
                                memory_space=pltpu.SMEM) for i in range(2)]
    return pl.pallas_call(
        pass_kernel,
        grid_spec=pltpu.PrefetchScalarGridSpec(
            num_scalar_prefetch=3, grid=(n_exp,),
            in_specs=x_specs + table_specs * 2 + [pl.BlockSpec(memory_space=ANY)] * (3 + len(after)),
            out_specs=[pl.BlockSpec(memory_space=ANY)] * 4,
            scratch_shapes=[pltpu.VMEM((2,) + w.shape[1:], jnp.bfloat16) for w in (wg, wu, wd)] +
                           [pltpu.VMEM((rows, ff), jnp.bfloat16),
                            pltpu.VMEM((rows, width), jnp.bfloat16),
                            pltpu.VMEM((rows // 8, 8 * width // LANES, LANES), jnp.float32),
                            pltpu.VMEM((4, acc_rows, LANES), jnp.float32),
                            pltpu.SemaphoreType.DMA((2, 3)),
                            pltpu.SemaphoreType.DMA((4,))]),
        out_shape=[acc] * 4,
        compiler_params=pltpu.CompilerParams(dimension_semantics=('arbitrary',), vmem_limit_bytes=67043328),
        cost_estimate=pl.CostEstimate(flops=2 * n_exp * rows * width * ff * 3, transcendentals=0,
                                      bytes_accessed=3 * n_exp * width * ff * 2),
        name='ffn_pass',
    )(src, core, count, x, x, addr, addr, wt, wt, wg, wu, wd, *after)


def final_kernel(a1_ref, a2_ref, b1_ref, b2_ref, *rest):
    out_ref, s_ref = rest[-2:]
    step = pl.program_id(0)
    half = pl.num_programs(0) // 2

    def emit(a_ref, b_ref):
        def body(b, carry):
            r = pl.ds(pl.multiple_of(b * 16 * JT, 16 * JT), 16 * JT)
            s_ref[r, :] = a_ref[r, :] + b_ref[r, :]
            for j in range(JT):
                pair = [s_ref[pl.ds((b * 16 + k) * JT + j, 8, stride=JT), :] for k in (0, 8)]
                out_ref[pl.ds(pl.multiple_of(b * 16, 16), 16), j * LANES:(j + 1) * LANES] = (
                    jnp.concatenate(pair, axis=0).astype(out_ref.dtype))
            return carry

        lax.fori_loop(0, out_ref.shape[0] // 16, body, 0)

    pl.when(step < half)(lambda: emit(a1_ref, b1_ref))
    pl.when(step >= half)(lambda: emit(a2_ref, b2_ref))


def final_sum(a1, a2, b1, b2, n, n_tok, width, out):
    tb = 128
    steps = n_tok // tb
    half = steps // 2
    low = pl.BlockSpec((tb * JT, LANES), lambda i: (jnp.minimum(i, half - 1), 0))
    high = pl.BlockSpec((tb * JT, LANES), lambda i: (jnp.maximum(i - half, 0), 0))
    prior = [] if out is None else [out]
    return pl.pallas_call(
        final_kernel,
        grid=(steps,),
        in_specs=[low, high, low, high] + [pl.BlockSpec(memory_space=ANY)] * len(prior),
        out_specs=pl.BlockSpec((tb, COLS), lambda i: (i, n)),
        scratch_shapes=[pltpu.VMEM((tb * JT, LANES), jnp.float32)],
        out_shape=jax.ShapeDtypeStruct((n_tok, width), jnp.bfloat16),
        input_output_aliases={4: 0} if prior else {},
        compiler_params=pltpu.CompilerParams(dimension_semantics=('arbitrary',), vmem_limit_bytes=30 * 2 ** 20),
        cost_estimate=pl.CostEstimate(flops=10 ** 7, transcendentals=0, bytes_accessed=n_tok * COLS * 10),
        name='final_sum',
    )(a1, a2, b1, b2, *prior)


def solution(mesh):
    token_spec = P(('dp',) + GROUP_AXES, None)
    weight_spec = P(GROUP_AXES, None, None)
    rows_spec = P('dp', GROUP_AXES, None, None)
    n_dev = mesh.shape['eo'] * mesh.shape['em'] * mesh.shape['ei']
    core_bit, x_bit, y_bit = 1, 2, 4
    to_pair = [(i, i ^ core_bit) for i in range(n_dev)]
    straight = [(i, i ^ (y_bit if i & core_bit else x_bit)) for i in range(n_dev)]
    crossed = [(i, i ^ (x_bit if i & core_bit else y_bit)) for i in range(n_dev)]

    def send(a, pairs):
        return lax.ppermute(a, GROUP_AXES, pairs)

    def local_part(x_local, w_gate, w_up, w_down, slot_idx, expert_idx, gate_wt):
        _, n_exp, slots, width = x_local.shape
        n_tok = slot_idx.shape[0]
        core = lax.axis_index('ei').astype(jnp.int32).reshape(1)
        chip = (lax.axis_index('eo') * 2 + lax.axis_index('em')).astype(jnp.int32)

        table = slot_tables(slot_idx, expert_idx, gate_wt, n_dev * n_exp, slots)
        table = table.reshape(2, n_dev, n_exp, slots).swapaxes(0, 1)
        table = lax.all_to_all(table, GROUP_AXES, 0, 0, tiled=True)
        addr = table[:, 0].astype(jnp.int32)
        wt = table[:, 1]
        seen = jnp.where(wt > 0, lax.broadcasted_iota(jnp.int32, wt.shape, 2) + 1, 0)
        count = jnp.max(seen, axis=2).reshape(-1)
        addr, wt = addr[:, :, None], wt[:, :, None]

        lo, hi = slice(0, n_tok // 2 * JT), slice(n_tok // 2 * JT, n_tok * JT)
        blocks = range(width // COLS)

        def ffn(flips, after):
            src = jnp.stack([2 * (chip ^ f) + i for i, f in enumerate(flips)])
            own0, sib0, own1, sib1 = ffn_pass(src, core, count, addr, wt, x_local, w_gate, w_up, w_down, n_tok, after)
            return [(own0, send(sib0, to_pair)), (own1, send(sib1, to_pair))]

        relay_lo, relay_hi, gate = [], [], []
        for n, (own, sib) in zip(blocks, ffn((3, 3), [])):
            low, high = own[lo] + sib[lo], own[hi] + sib[hi]
            relay_lo.append(send(low, straight))
            relay_hi.append(send(high, crossed))
            gate.append(low)

        got, got2, after2 = [], [], []
        for n, (own, sib) in zip(blocks, ffn((1, 2), gate)):
            low = own[lo] + sib[lo]
            own, sib, relayed = lax.optimization_barrier((own, sib, relay_hi[n]))
            got.append((send(low, straight),
                        send(own[hi] + sib[hi] + relayed, straight)))
            after2.append(low)
        for n, (own, sib) in zip(blocks, ffn((2, 1), after2)):
            high = own[hi] + sib[hi]
            own, sib, relayed = lax.optimization_barrier((own, sib, relay_lo[n]))
            got2.append((send(own[lo] + sib[lo] + relayed, crossed),
                         send(high, crossed)))
            gate = [high]

        out = None
        for n, (own, sib) in zip(blocks, ffn((0, 0), gate)):
            out = final_sum(own[lo] + sib[lo] + got[n][0], own[hi] + sib[hi] + got[n][1],
                            got2[n][0], got2[n][1], n, n_tok, width, out)
        return out

    return jax.shard_map(local_part, mesh=mesh,
                         in_specs=(rows_spec, weight_spec, weight_spec, weight_spec, token_spec, token_spec, token_spec),
                         out_specs=token_spec, check_vma=False)
```

```python
import functools

import jax
import jax.numpy as jnp
from jax import lax
from jax.experimental import pallas as pl
from jax.experimental.pallas import tpu as pltpu
from jax.sharding import PartitionSpec as P


GROUP_AXES = ('eo', 'em', 'ei')
LANES = 128
COLS = 1024
JT = COLS // LANES
ANY = pl.ANY


def slot_tables(slot_idx, expert_idx, gate_wt, n_exp, n_slot):
    n_tok, top = slot_idx.shape
    tok = lax.broadcasted_iota(jnp.int32, (n_tok, top), 0)
    spare = float(n_tok * JT)
    delta = (tok * JT).astype(jnp.float32) - spare
    exp_hot = (expert_idx[:, :, None] == lax.broadcasted_iota(jnp.int32, (1, 1, n_exp), 2)).astype(jnp.float32)
    slot_hot = (slot_idx[:, :, None] == lax.broadcasted_iota(jnp.int32, (1, 1, n_slot), 2)).astype(jnp.float32)
    both = jnp.concatenate([exp_hot * delta[:, :, None], exp_hot * gate_wt[:, :, None]], axis=2)
    table = jnp.einsum('tje,tjc->ec', both, slot_hot, precision=lax.Precision.HIGHEST,
                       preferred_element_type=jnp.float32)
    addr, wt = table[:n_exp] + spare, table[n_exp:]
    return jnp.stack([addr, wt])


def round16(n):
    return (n + 15) // 16 * 16


def row_chunks(total, body):
    whole = (total + 127) // 256
    rest = total - whole * 256

    def chunk(c, carry):
        body(pl.multiple_of(c * 256, 256), 256)
        return carry

    lax.fori_loop(0, whole, chunk, 0)
    pl.when(rest > 0)(lambda: body(pl.multiple_of(whole * 256, 256), 128))


def gate_up_tile(x, wg_ref, wu_ref, cols):
    w = jnp.concatenate([wg_ref[:, cols], wu_ref[:, cols]], axis=1)
    gu = jnp.dot(x, w, preferred_element_type=jnp.float32)
    g, u = gu[:, :LANES], gu[:, LANES:]
    return ((g * jax.nn.sigmoid(g)) * u).astype(jnp.bfloat16)


def pass_kernel(src_ref, core_ref, n_ref, *refs):
    x_refs, addr_refs, wt_refs, weights = refs[0:2], refs[2:4], refs[4:6], refs[6:9]
    outs, bufs, (h_ref, xs_ref, y_ref, acc_ref, w_sem, sem) = refs[-13:-9], refs[-9:-6], refs[-6:]
    ff = h_ref.shape[1]
    e = pl.program_id(0)
    n_exp = pl.num_programs(0)
    slot = e % 2

    def fetch(k, expert, into):
        return pltpu.make_async_copy(weights[k].at[expert], bufs[k].at[into], w_sem.at[into, k])

    @pl.when(e == 0)
    def _():
        for k in range(3):
            fetch(k, 0, 0).start()

    def fetch_next(ks):
        @pl.when(e + 1 < n_exp)
        def _():
            for k in ks:
                fetch(k, e + 1, 1 - slot).start()

    @pl.when(e == 0)
    def _():
        def zero(i, carry):
            r = pl.ds(pl.multiple_of(i * 8 * JT, 8 * JT), 8 * JT)
            for k in range(acc_ref.shape[0]):
                acc_ref[k, r, :] = jnp.zeros((8 * JT, LANES), jnp.float32)
            return carry

        lax.fori_loop(0, acc_ref.shape[1] // (8 * JT), zero, 0)

    counts = [n_ref[src_ref[i] * n_exp + e] for i in range(2)]
    first = [jnp.int32(0), round16(counts[0])]
    total = first[1] + round16(counts[1])

    for i in range(2):
        def copy(b, carry):
            xs_ref[pl.ds(pl.multiple_of(first[i] + b * 16, 16), 16), :] = (
                x_refs[i][0, 0, pl.ds(pl.multiple_of(b * 16, 16), 16), :])
            return carry

        lax.fori_loop(0, round16(counts[i]) // 16, copy, 0)

    fetch(0, e, slot).wait()
    fetch(1, e, slot).wait()
    fetch_next((0, 1))
    wg_ref, wu_ref, wd_ref = (buf.at[slot] for buf in bufs)

    def hidden(r0, rows):
        r = pl.ds(r0, rows)
        for j in range(ff // LANES):
            cols = slice(j * LANES, (j + 1) * LANES)
            h_ref[r, cols] = gate_up_tile(xs_ref[r, :], wg_ref, wu_ref, cols)

    row_chunks(total, hidden)
    fetch(2, e, slot).wait()
    fetch_next((2,))

    def result(r0, rows):
        for jj in range(wd_ref.shape[1] // 256):
            y = jnp.dot(h_ref[pl.ds(r0, rows), :], wd_ref[:, jj * 256:(jj + 1) * 256],
                        preferred_element_type=jnp.float32)
            y = y.astype(jnp.bfloat16).astype(jnp.float32)
            for k in range(2):
                y_ref[pl.ds(r0 // 8, rows // 8), (jj * 2 + k) * 8:(jj * 2 + k + 1) * 8, :] = (
                    y[:, k * LANES:(k + 1) * LANES].reshape(rows // 8, 8, LANES))

    row_chunks(total, result)

    for i in range(2):
        y0 = first[i] // 8

        def batch(b, carry):
            at = [pl.ds(pl.multiple_of(addr_refs[i][0, 0, 0, b * 8 + k], JT), JT) for k in range(8)]
            wts = [wt_refs[i][0, 0, 0, b * 8 + k] for k in range(8)]
            work = [(k, col) for k in range(8) for col in range(2)]
            ys = [y_ref[y0 + b, pl.ds(col * 8 * JT + k, JT, stride=8), :] for k, col in work]
            old = [acc_ref[col * 2 + i, at[k], :] for k, col in work]
            for (k, col), y, a in zip(work, ys, old):
                acc_ref[col * 2 + i, at[k], :] = a + wts[k] * y
            return carry

        lax.fori_loop(0, (counts[i] + 7) // 8, batch, 0)

    @pl.when(e == n_exp - 1)
    def _():
        copies = []
        for col in range(2):
            for i in range(2):
                own = core_ref[0] == i
                k = col * 2 + i
                for dst, cond in ((outs[col * 2], own), (outs[col * 2 + 1], jnp.logical_not(own))):
                    copies.append((cond, pltpu.make_async_copy(acc_ref.at[k], dst, sem.at[k])))
        for cond, copy in copies:
            pl.when(cond)(copy.start)
        for cond, copy in copies:
            pl.when(cond)(copy.wait)


def ffn_pass(src, core, count, addr, wt, x, wg, wu, wd, n_tok, after):
    _, n_exp, slots, width = x.shape
    ff = wg.shape[2]
    rows = 2 * slots
    acc_rows = (n_tok + 8) * JT
    acc = jax.ShapeDtypeStruct((acc_rows, LANES), jnp.float32)
    x_specs = [pl.BlockSpec((1, 1, slots, width), lambda e, src, *_, i=i: (src[i], e, 0, 0)) for i in range(2)]
    table_specs = [pl.BlockSpec((1, 1, 1, slots), lambda e, src, *_, i=i: (src[i], e, 0, 0),
                                memory_space=pltpu.SMEM) for i in range(2)]
    return pl.pallas_call(
        pass_kernel,
        grid_spec=pltpu.PrefetchScalarGridSpec(
            num_scalar_prefetch=3, grid=(n_exp,),
            in_specs=x_specs + table_specs * 2 + [pl.BlockSpec(memory_space=ANY)] * (3 + len(after)),
            out_specs=[pl.BlockSpec(memory_space=ANY)] * 4,
            scratch_shapes=[pltpu.VMEM((2,) + w.shape[1:], jnp.bfloat16) for w in (wg, wu, wd)] +
                           [pltpu.VMEM((rows, ff), jnp.bfloat16),
                            pltpu.VMEM((rows, width), jnp.bfloat16),
                            pltpu.VMEM((rows // 8, 8 * width // LANES, LANES), jnp.float32),
                            pltpu.VMEM((4, acc_rows, LANES), jnp.float32),
                            pltpu.SemaphoreType.DMA((2, 3)),
                            pltpu.SemaphoreType.DMA((4,))]),
        out_shape=[acc] * 4,
        compiler_params=pltpu.CompilerParams(dimension_semantics=('arbitrary',), vmem_limit_bytes=67043328),
        cost_estimate=pl.CostEstimate(flops=2 * n_exp * rows * width * ff * 3, transcendentals=0,
                                      bytes_accessed=3 * n_exp * width * ff * 2),
        name='ffn_pass',
    )(src, core, count, x, x, addr, addr, wt, wt, wg, wu, wd, *after)


def chip_sum_kernel(low_half, own_ref, sib_ref, relay_ref, out_ref):
    in_low = pl.program_id(0) < pl.num_programs(0) // 2
    relayed = in_low if low_half else jnp.logical_not(in_low)

    @pl.when(relayed)
    def _():
        out_ref[...] = own_ref[...] + sib_ref[...] + relay_ref[...]

    @pl.when(jnp.logical_not(relayed))
    def _():
        out_ref[...] = own_ref[...] + sib_ref[...]


def chip_sum(own, sib, relay, low_half):
    rows = 2 * relay.shape[0]
    steps = 2
    block = rows // steps
    half = steps // 2
    if low_half:
        relay_map = lambda t: (jnp.minimum(t, half - 1), 0)
    else:
        relay_map = lambda t: (jnp.maximum(t - half, 0), 0)
    spec = pl.BlockSpec((block, LANES), lambda t: (t, 0))
    return pl.pallas_call(
        functools.partial(chip_sum_kernel, low_half),
        grid=(steps,),
        in_specs=[spec, spec, pl.BlockSpec((block, LANES), relay_map)],
        out_specs=spec,
        out_shape=jax.ShapeDtypeStruct((rows, LANES), jnp.float32),
        compiler_params=pltpu.CompilerParams(dimension_semantics=('arbitrary',), vmem_limit_bytes=60 * 2 ** 20),
        cost_estimate=pl.CostEstimate(flops=10 ** 7, transcendentals=0, bytes_accessed=rows * LANES * 14),
        name='chip_sum',
    )(own, sib, relay)


def final_kernel(a_ref, b_ref, *rest):
    out_ref, s_ref = rest[-2:]

    def body(b, carry):
        r = pl.ds(pl.multiple_of(b * 16 * JT, 16 * JT), 16 * JT)
        s_ref[r, :] = a_ref[r, :] + b_ref[r, :]
        for j in range(JT):
            pair = [s_ref[pl.ds((b * 16 + k) * JT + j, 8, stride=JT), :] for k in (0, 8)]
            out_ref[pl.ds(pl.multiple_of(b * 16, 16), 16), j * LANES:(j + 1) * LANES] = (
                jnp.concatenate(pair, axis=0).astype(out_ref.dtype))
        return carry

    lax.fori_loop(0, out_ref.shape[0] // 16, body, 0, unroll=4)


def final_sum(a, b, n, n_tok, width, out):
    tb = 256
    spec = pl.BlockSpec((tb * JT, LANES), lambda i: (i, 0))
    prior = [] if out is None else [out]
    return pl.pallas_call(
        final_kernel,
        grid=(n_tok // tb,),
        in_specs=[spec, spec] + [pl.BlockSpec(memory_space=ANY)] * len(prior),
        out_specs=pl.BlockSpec((tb, COLS), lambda i: (i, n)),
        scratch_shapes=[pltpu.VMEM((tb * JT, LANES), jnp.float32)],
        out_shape=jax.ShapeDtypeStruct((n_tok, width), jnp.bfloat16),
        input_output_aliases={2: 0} if prior else {},
        compiler_params=pltpu.CompilerParams(dimension_semantics=('arbitrary',), vmem_limit_bytes=30 * 2 ** 20),
        cost_estimate=pl.CostEstimate(flops=10 ** 7, transcendentals=0, bytes_accessed=n_tok * COLS * 10),
        name='final_sum',
    )(a, b, *prior)


def solution(mesh):
    token_spec = P(('dp',) + GROUP_AXES, None)
    weight_spec = P(GROUP_AXES, None, None)
    rows_spec = P('dp', GROUP_AXES, None, None)
    n_dev = mesh.shape['eo'] * mesh.shape['em'] * mesh.shape['ei']
    core_bit, x_bit, y_bit = 1, 2, 4
    to_pair = [(i, i ^ core_bit) for i in range(n_dev)]
    straight = [(i, i ^ (y_bit if i & core_bit else x_bit)) for i in range(n_dev)]
    crossed = [(i, i ^ (x_bit if i & core_bit else y_bit)) for i in range(n_dev)]

    def send(a, pairs):
        return lax.ppermute(a, GROUP_AXES, pairs)

    def local_part(x_local, w_gate, w_up, w_down, slot_idx, expert_idx, gate_wt):
        _, n_exp, slots, width = x_local.shape
        n_tok = slot_idx.shape[0]
        core = lax.axis_index('ei').astype(jnp.int32).reshape(1)
        chip = (lax.axis_index('eo') * 2 + lax.axis_index('em')).astype(jnp.int32)

        table = slot_tables(slot_idx, expert_idx, gate_wt, n_dev * n_exp, slots)
        table = table.reshape(2, n_dev, n_exp, slots).swapaxes(0, 1)
        table = lax.all_to_all(table, GROUP_AXES, 0, 0, tiled=True)
        addr = table[:, 0].astype(jnp.int32)
        wt = table[:, 1]
        seen = jnp.where(wt > 0, lax.broadcasted_iota(jnp.int32, wt.shape, 2) + 1, 0)
        count = jnp.max(seen, axis=2).reshape(-1)
        addr, wt = addr[:, :, None], wt[:, :, None]

        lo, hi = slice(0, n_tok // 2 * JT), slice(n_tok // 2 * JT, n_tok * JT)
        blocks = range(width // COLS)

        def ffn(flips, after):
            src = jnp.stack([2 * (chip ^ f) + i for i, f in enumerate(flips)])
            own0, sib0, own1, sib1 = ffn_pass(src, core, count, addr, wt, x_local, w_gate, w_up, w_down, n_tok, after)
            return [(own0, send(sib0, to_pair)), (own1, send(sib1, to_pair))]

        relay_lo, relay_hi, gate = [], [], []
        for n, (own, sib) in zip(blocks, ffn((3, 3), [])):
            low, high = own[lo] + sib[lo], own[hi] + sib[hi]
            relay_lo.append(send(low, straight))
            relay_hi.append(send(high, crossed))
            gate.append(low)

        got, got2, after2 = [], [], []
        for n, (own, sib) in zip(blocks, ffn((1, 2), gate)):
            total = chip_sum(own, sib, relay_hi[n], False)
            got.append(send(total, straight))
            after2.append(total)
        gate = []
        for n, (own, sib) in zip(blocks, ffn((2, 1), after2)):
            total = chip_sum(own, sib, relay_lo[n], True)
            got2.append(send(total, crossed))
            gate.append(total)

        out = None
        for n, (own, sib) in zip(blocks, ffn((0, 0), gate)):
            early = own[:n_tok * JT] + sib[:n_tok * JT] + got[n]
            out = final_sum(early, got2[n], n, n_tok, width, out)
        return out

    return jax.shard_map(local_part, mesh=mesh,
                         in_specs=(rows_spec, weight_spec, weight_spec, weight_spec, token_spec, token_spec, token_spec),
                         out_specs=token_spec, check_vma=False)
```

```python
import functools

import jax
import jax.numpy as jnp
from jax import lax
from jax.experimental import pallas as pl
from jax.experimental.pallas import tpu as pltpu
from jax.sharding import PartitionSpec as P


GROUP_AXES = ('eo', 'em', 'ei')
LANES = 128
COLS = 1024
JT = COLS // LANES
ANY = pl.ANY


def slot_tables(slot_idx, expert_idx, gate_wt, n_exp, n_slot):
    n_tok, top = slot_idx.shape
    tok = lax.broadcasted_iota(jnp.int32, (n_tok, top), 0)
    spare = float(n_tok * JT)
    delta = (tok * JT).astype(jnp.float32) - spare
    exp_hot = (expert_idx[:, :, None] == lax.broadcasted_iota(jnp.int32, (1, 1, n_exp), 2)).astype(jnp.float32)
    slot_hot = (slot_idx[:, :, None] == lax.broadcasted_iota(jnp.int32, (1, 1, n_slot), 2)).astype(jnp.float32)
    both = jnp.concatenate([exp_hot * delta[:, :, None], exp_hot * gate_wt[:, :, None]], axis=2)
    table = jnp.einsum('tje,tjc->ec', both, slot_hot, precision=lax.Precision.HIGHEST,
                       preferred_element_type=jnp.float32)
    addr, wt = table[:n_exp] + spare, table[n_exp:]
    return jnp.stack([addr, wt])


def round16(n):
    return (n + 15) // 16 * 16


def row_chunks(total, body):
    whole = (total + 127) // 256
    rest = total - whole * 256

    def chunk(c, carry):
        body(pl.multiple_of(c * 256, 256), 256)
        return carry

    lax.fori_loop(0, whole, chunk, 0)
    pl.when(rest > 0)(lambda: body(pl.multiple_of(whole * 256, 256), 128))


def gate_up_tile(x, wg_ref, wu_ref, cols):
    w = jnp.concatenate([wg_ref[:, cols], wu_ref[:, cols]], axis=1)
    gu = jnp.dot(x, w, preferred_element_type=jnp.float32)
    g, u = gu[:, :LANES], gu[:, LANES:]
    return ((g * jax.nn.sigmoid(g)) * u).astype(jnp.bfloat16)


def pass_kernel(src_ref, core_ref, n_ref, *refs):
    x_ref, addr_refs, wt_refs, weights = refs[0], refs[1:3], refs[3:5], refs[5:8]
    outs, bufs, (x_buf, h_ref, xs_ref, y_ref, acc_ref, w_sem, sem) = refs[-14:-10], refs[-10:-7], refs[-7:]
    ff = h_ref.shape[1]
    e = pl.program_id(0)
    n_exp = pl.num_programs(0)
    slot = e % 2

    def fetch(k, expert, into):
        if k >= 3:
            return pltpu.make_async_copy(x_ref.at[src_ref[k - 3], expert], x_buf.at[into, k - 3], w_sem.at[into, k])
        return pltpu.make_async_copy(weights[k].at[expert], bufs[k].at[into], w_sem.at[into, k])

    @pl.when(e == 0)
    def _():
        for k in (3, 4, 0, 1, 2):
            fetch(k, 0, 0).start()

    def fetch_next(ks):
        @pl.when(e + 1 < n_exp)
        def _():
            for k in ks:
                fetch(k, e + 1, 1 - slot).start()

    @pl.when(e == 0)
    def _():
        def zero(i, carry):
            r = pl.ds(pl.multiple_of(i * 8 * JT, 8 * JT), 8 * JT)
            for k in range(acc_ref.shape[0]):
                acc_ref[k, r, :] = jnp.zeros((8 * JT, LANES), jnp.float32)
            return carry

        lax.fori_loop(0, acc_ref.shape[1] // (8 * JT), zero, 0)

    counts = [n_ref[src_ref[i] * n_exp + e] for i in range(2)]
    first = [jnp.int32(0), round16(counts[0])]
    total = first[1] + round16(counts[1])

    for i in range(2):
        fetch(3 + i, e, slot).wait()

        def copy(b, carry):
            xs_ref[pl.ds(pl.multiple_of(first[i] + b * 16, 16), 16), :] = (
                x_buf[slot, i, pl.ds(pl.multiple_of(b * 16, 16), 16), :])
            return carry

        lax.fori_loop(0, round16(counts[i]) // 16, copy, 0)

    fetch(0, e, slot).wait()
    fetch(1, e, slot).wait()
    fetch_next((3, 4, 0, 1))
    wg_ref, wu_ref, wd_ref = (buf.at[slot] for buf in bufs)

    def hidden(r0, rows):
        r = pl.ds(r0, rows)
        for j in range(ff // LANES):
            cols = slice(j * LANES, (j + 1) * LANES)
            h_ref[r, cols] = gate_up_tile(xs_ref[r, :], wg_ref, wu_ref, cols)

    row_chunks(total, hidden)
    fetch(2, e, slot).wait()
    fetch_next((2,))

    def result(r0, rows):
        for jj in range(wd_ref.shape[1] // 256):
            y = jnp.dot(h_ref[pl.ds(r0, rows), :], wd_ref[:, jj * 256:(jj + 1) * 256],
                        preferred_element_type=jnp.float32)
            y = y.astype(jnp.bfloat16).astype(jnp.float32)
            for k in range(2):
                y_ref[pl.ds(r0 // 8, rows // 8), (jj * 2 + k) * 8:(jj * 2 + k + 1) * 8, :] = (
                    y[:, k * LANES:(k + 1) * LANES].reshape(rows // 8, 8, LANES))

    row_chunks(total, result)

    for i in range(2):
        y0 = first[i] // 8

        def batch(b, carry):
            at = [pl.ds(pl.multiple_of(addr_refs[i][0, 0, 0, b * 8 + k], JT), JT) for k in range(8)]
            wts = [wt_refs[i][0, 0, 0, b * 8 + k] for k in range(8)]
            work = [(k, col) for k in range(8) for col in range(2)]
            ys = [y_ref[y0 + b, pl.ds(col * 8 * JT + k, JT, stride=8), :] for k, col in work]
            old = [acc_ref[col * 2 + i, at[k], :] for k, col in work]
            for (k, col), y, a in zip(work, ys, old):
                acc_ref[col * 2 + i, at[k], :] = a + wts[k] * y
            return carry

        lax.fori_loop(0, (counts[i] + 7) // 8, batch, 0)

    @pl.when(e == n_exp - 1)
    def _():
        copies = []
        for col in range(2):
            for i in range(2):
                own = core_ref[0] == i
                k = col * 2 + i
                for dst, cond in ((outs[col * 2], own), (outs[col * 2 + 1], jnp.logical_not(own))):
                    copies.append((cond, pltpu.make_async_copy(acc_ref.at[k], dst, sem.at[k])))
        for cond, copy in copies:
            pl.when(cond)(copy.start)
        for cond, copy in copies:
            pl.when(cond)(copy.wait)


def ffn_pass(src, core, count, addr, wt, x, wg, wu, wd, n_tok, after):
    _, n_exp, slots, width = x.shape
    ff = wg.shape[2]
    rows = 2 * slots
    acc_rows = (n_tok + 8) * JT
    acc = jax.ShapeDtypeStruct((acc_rows, LANES), jnp.float32)
    table_specs = [pl.BlockSpec((1, 1, 1, slots), lambda e, src, *_, i=i: (src[i], e, 0, 0),
                                memory_space=pltpu.SMEM) for i in range(2)]
    return pl.pallas_call(
        pass_kernel,
        grid_spec=pltpu.PrefetchScalarGridSpec(
            num_scalar_prefetch=3, grid=(n_exp,),
            in_specs=[pl.BlockSpec(memory_space=ANY)] + table_specs * 2 + [pl.BlockSpec(memory_space=ANY)] * (3 + len(after)),
            out_specs=[pl.BlockSpec(memory_space=ANY)] * 4,
            scratch_shapes=[pltpu.VMEM((2,) + w.shape[1:], jnp.bfloat16) for w in (wg, wu, wd)] +
                           [pltpu.VMEM((2, 2, slots, width), jnp.bfloat16),
                            pltpu.VMEM((rows, ff), jnp.bfloat16),
                            pltpu.VMEM((rows, width), jnp.bfloat16),
                            pltpu.VMEM((rows // 8, 8 * width // LANES, LANES), jnp.float32),
                            pltpu.VMEM((4, acc_rows, LANES), jnp.float32),
                            pltpu.SemaphoreType.DMA((2, 5)),
                            pltpu.SemaphoreType.DMA((4,))]),
        out_shape=[acc] * 4,
        compiler_params=pltpu.CompilerParams(dimension_semantics=('arbitrary',), vmem_limit_bytes=67043328),
        cost_estimate=pl.CostEstimate(flops=2 * n_exp * rows * width * ff * 3, transcendentals=0,
                                      bytes_accessed=3 * n_exp * width * ff * 2),
        name='ffn_pass',
    )(src, core, count, x, addr, addr, wt, wt, wg, wu, wd, *after)


def chip_sum_kernel(low_half, own_ref, sib_ref, relay_ref, out_ref):
    in_low = pl.program_id(0) < pl.num_programs(0) // 2
    relayed = in_low if low_half else jnp.logical_not(in_low)

    @pl.when(relayed)
    def _():
        out_ref[...] = own_ref[...] + sib_ref[...] + relay_ref[...]

    @pl.when(jnp.logical_not(relayed))
    def _():
        out_ref[...] = own_ref[...] + sib_ref[...]


def chip_sum(own, sib, relay, low_half):
    rows = 2 * relay.shape[0]
    steps = 2
    block = rows // steps
    half = steps // 2
    if low_half:
        relay_map = lambda t: (jnp.minimum(t, half - 1), 0)
    else:
        relay_map = lambda t: (jnp.maximum(t - half, 0), 0)
    spec = pl.BlockSpec((block, LANES), lambda t: (t, 0))
    return pl.pallas_call(
        functools.partial(chip_sum_kernel, low_half),
        grid=(steps,),
        in_specs=[spec, spec, pl.BlockSpec((block, LANES), relay_map)],
        out_specs=spec,
        out_shape=jax.ShapeDtypeStruct((rows, LANES), jnp.float32),
        compiler_params=pltpu.CompilerParams(dimension_semantics=('arbitrary',), vmem_limit_bytes=60 * 2 ** 20),
        cost_estimate=pl.CostEstimate(flops=10 ** 7, transcendentals=0, bytes_accessed=rows * LANES * 14),
        name='chip_sum',
    )(own, sib, relay)


def final_kernel(own_ref, sib_ref, a_ref, b_ref, *rest):
    out_ref, s_ref = rest[-2:]

    def body(b, carry):
        r = pl.ds(pl.multiple_of(b * 16 * JT, 16 * JT), 16 * JT)
        s_ref[r, :] = (own_ref[r, :] + sib_ref[r, :]) + (a_ref[r, :] + b_ref[r, :])
        for j in range(JT):
            pair = [s_ref[pl.ds((b * 16 + k) * JT + j, 8, stride=JT), :] for k in (0, 8)]
            out_ref[pl.ds(pl.multiple_of(b * 16, 16), 16), j * LANES:(j + 1) * LANES] = (
                jnp.concatenate(pair, axis=0).astype(out_ref.dtype))
        return carry

    lax.fori_loop(0, out_ref.shape[0] // 16, body, 0, unroll=4)


def final_sum(parts, n, n_tok, width, out):
    tb = 256
    spec = pl.BlockSpec((tb * JT, LANES), lambda i: (i, 0))
    prior = [] if out is None else [out]
    return pl.pallas_call(
        final_kernel,
        grid=(n_tok // tb,),
        in_specs=[spec] * len(parts) + [pl.BlockSpec(memory_space=ANY)] * len(prior),
        out_specs=pl.BlockSpec((tb, COLS), lambda i: (i, n)),
        scratch_shapes=[pltpu.VMEM((tb * JT, LANES), jnp.float32)],
        out_shape=jax.ShapeDtypeStruct((n_tok, width), jnp.bfloat16),
        input_output_aliases={len(parts): 0} if prior else {},
        compiler_params=pltpu.CompilerParams(dimension_semantics=('arbitrary',), vmem_limit_bytes=30 * 2 ** 20),
        cost_estimate=pl.CostEstimate(flops=10 ** 7, transcendentals=0, bytes_accessed=n_tok * COLS * 18),
        name='final_sum',
    )(*parts, *prior)


def solution(mesh):
    token_spec = P(('dp',) + GROUP_AXES, None)
    weight_spec = P(GROUP_AXES, None, None)
    rows_spec = P('dp', GROUP_AXES, None, None)
    n_dev = mesh.shape['eo'] * mesh.shape['em'] * mesh.shape['ei']
    core_bit, x_bit, y_bit = 1, 2, 4
    to_pair = [(i, i ^ core_bit) for i in range(n_dev)]
    straight = [(i, i ^ (y_bit if i & core_bit else x_bit)) for i in range(n_dev)]
    crossed = [(i, i ^ (x_bit if i & core_bit else y_bit)) for i in range(n_dev)]

    def send(a, pairs):
        return lax.ppermute(a, GROUP_AXES, pairs)

    def local_part(x_local, w_gate, w_up, w_down, slot_idx, expert_idx, gate_wt):
        _, n_exp, slots, width = x_local.shape
        n_tok = slot_idx.shape[0]
        core = lax.axis_index('ei').astype(jnp.int32).reshape(1)
        chip = (lax.axis_index('eo') * 2 + lax.axis_index('em')).astype(jnp.int32)

        table = slot_tables(slot_idx, expert_idx, gate_wt, n_dev * n_exp, slots)
        table = table.reshape(2, n_dev, n_exp, slots).swapaxes(0, 1)
        table = lax.all_to_all(table, GROUP_AXES, 0, 0, tiled=True)
        addr = table[:, 0].astype(jnp.int32)
        wt = table[:, 1]
        seen = jnp.where(wt > 0, lax.broadcasted_iota(jnp.int32, wt.shape, 2) + 1, 0)
        count = jnp.max(seen, axis=2).reshape(-1)
        addr, wt = addr[:, :, None], wt[:, :, None]

        lo, hi = slice(0, n_tok // 2 * JT), slice(n_tok // 2 * JT, n_tok * JT)
        blocks = range(width // COLS)

        def ffn(flips, after):
            src = jnp.stack([2 * (chip ^ f) + i for i, f in enumerate(flips)])
            own0, sib0, own1, sib1 = ffn_pass(src, core, count, addr, wt, x_local, w_gate, w_up, w_down, n_tok, after)
            return [(own0, send(sib0, to_pair)), (own1, send(sib1, to_pair))]

        relay_lo, relay_hi, gate = [], [], []
        for n, (own, sib) in zip(blocks, ffn((3, 3), [])):
            low, high = own[lo] + sib[lo], own[hi] + sib[hi]
            relay_lo.append(send(low, straight))
            relay_hi.append(send(high, crossed))
            gate.append(low)

        got, got2, after2 = [], [], []
        for n, (own, sib) in zip(blocks, ffn((1, 2), gate)):
            total = chip_sum(own, sib, relay_hi[n], False)
            got.append(send(total, straight))
            after2.append(total)
        gate = []
        for n, (own, sib) in zip(blocks, ffn((2, 1), after2)):
            total = chip_sum(own, sib, relay_lo[n], True)
            got2.append(send(total, crossed))
            gate.append(total)

        out = None
        for n, (own, sib) in zip(blocks, ffn((0, 0), gate)):
            out = final_sum((own, sib, got[n], got2[n]), n, n_tok, width, out)
        return out

    return jax.shard_map(local_part, mesh=mesh,
                         in_specs=(rows_spec, weight_spec, weight_spec, weight_spec, token_spec, token_spec, token_spec),
                         out_specs=token_spec, check_vma=False)
```
